32 devices in a mesh: dp: 16 (over z, y, x), mp: 2 (over core).
Axes of the slice: x: 2, y: 2, z: 4, core: 2. Of those that a mesh axis runs over, the one named last changes fastest.
Arguments:
- hidden: bfloat16 [24576, 3584], P('dp', 'mp'), may hold values from -6 to 6
- frozen_value_weight: bfloat16 [3584, 512], P('mp'), may hold values from -0.09375 to 0.09375
- adapter_down_weight: bfloat16 [16, 3584, 32], P('dp', 'mp'), may hold values from -0.09375 to 0.09375
- adapter_up_weight: bfloat16 [16, 32, 512], P('dp', None, 'mp'), may hold values from -1 to 1
- value_output_gradient: bfloat16 [24576, 512], P('dp', 'mp'), may hold values from -6 to 6
- sequence_tenant_index: int32 [32], P('dp'), may hold values from 0 to 15
- tenant_slot_table: int32 [16], replicated, may hold values from 0 to 15, each once
Outputs:
- values: bfloat16 [24576, 512], P('dp', 'mp')
- hidden_grad: bfloat16 [24576, 3584], P('dp', 'mp')
- down_grad: float32 [16, 3584, 32], P('dp', 'mp')
- up_grad: float32 [16, 32, 512], P('dp', None, 'mp')
The draws below stay inside these ranges and needn't reach their ends.
Inputs may be any that keep to these rules, and one draw needn't show every extreme that they name: `sequence_tenant_index`: tenant of each sequence; several sequences may share a tenant. `tenant_slot_table`: every slot holds exactly one tenant.
All inputs are finite; a program needn't handle non-finite values.
Results may differ from the reference program's by a relative error of at most 0.0039.
Values may be sent and summed in bfloat16 or wider, within the bound.
No kernel may reach another device: no remote copies, remote signals or barrier semaphores. Data moves between devices by JAX's collectives and lax.ppermute only.
A program may use at most 128 MiB of HBM per device.

```python
import math
import jax
import jax.numpy as jnp
import numpy as np
from jax import lax

MODEL_WIDTH = 3584
VALUE_FEATURES = 512
ADAPTER_RANK = 32
LEN = 768
TENANT_SLOTS = 16
SEQS = 32
TOKENS = 24576


def set_ends(entries, own_key, smallest, largest):
    spot = [jax.random.randint(jax.random.fold_in(own_key, axis), (), 0, length) for axis, length in enumerate(entries.shape)]
    widest = entries.shape.index(max(entries.shape))
    beside = spot[:widest] + [(spot[widest] + 1) % entries.shape[widest]] + spot[widest + 1:]
    return entries.at[tuple(spot)].set(smallest).at[tuple(beside)].set(largest)


def shard_levels(own_key, extent, pieces, least, largest):
    gain = 1.0
    for axis_at, blocks in pieces:
        heights = jax.random.uniform(jax.random.fold_in(jax.random.fold_in(own_key, 6), axis_at), (blocks,), jnp.float32, least / len(pieces), largest / len(pieces))
        gain = gain * jnp.repeat(jnp.exp(heights), extent[axis_at] // blocks).reshape((-1,) + (1,) * (len(extent) - 1 - axis_at))
    return gain


def cumulative_ranks(count, skew):
    loads = [(1 << 20) // math.isqrt(rank ** skew) + 1 for rank in range(1, count + 1)]
    scale = 1 + sum(loads) // (1 << 30)
    return np.cumsum(np.array([max(1, weight // scale) for weight in loads]))


def skewed_ids(own_key, dims, amount, slope):
    listing = cumulative_ranks(amount, slope)
    ticket = jax.random.randint(jax.random.fold_in(own_key, 1), dims, 0, int(listing[amount - 1]))
    rank = jnp.searchsorted(jnp.asarray(listing, jnp.int32), ticket, side="right")
    return jax.random.permutation(jax.random.fold_in(own_key, 2), amount)[rank].astype(jnp.int32)


def scatter_about(own_key, extent, spread, most, cuts=(), kind=jnp.bfloat16):
    loudness = shard_levels(own_key, extent, cuts, -0.22, 0.18) if cuts else 1.0
    drawn = jax.random.normal(own_key, extent, jnp.float32) * spread * loudness
    return jnp.minimum(jnp.maximum(drawn, -most), most).astype(kind)


def setup_inputs(seed: int = 0) -> dict:
    seeds = jax.random.split(jax.random.key(seed), 8)
    return {
        "hidden": scatter_about(seeds[0], (TOKENS, MODEL_WIDTH), 1.0, 6.0, ((0, 16), (1, 2))),
        "frozen_value_weight": scatter_about(seeds[1], (MODEL_WIDTH, VALUE_FEATURES), MODEL_WIDTH ** -0.5, 0.09375, ((0, 2),)),
        "adapter_down_weight": scatter_about(seeds[2], (TENANT_SLOTS, MODEL_WIDTH, ADAPTER_RANK), MODEL_WIDTH ** -0.5, 0.09375, ((0, 16), (1, 2))),
        "adapter_up_weight": scatter_about(seeds[3], (TENANT_SLOTS, ADAPTER_RANK, VALUE_FEATURES), ADAPTER_RANK ** -0.5, 1.0, ((0, 16), (2, 2))),
        "value_output_gradient": scatter_about(seeds[4], (TOKENS, VALUE_FEATURES), 1.0, 6.0, ((0, 16), (1, 2))),
        "sequence_tenant_index": set_ends(skewed_ids(seeds[5], (SEQS,), TENANT_SLOTS, 2), jax.random.fold_in(seeds[5], 3), 0, TENANT_SLOTS - 1).astype(jnp.int32),
        "tenant_slot_table": jax.random.permutation(seeds[6], TENANT_SLOTS).astype(jnp.int32),
    }


highest_precision = lax.Precision.HIGHEST


def reference(hidden, frozen_value_weight, adapter_down_weight, adapter_up_weight, value_output_gradient, sequence_tenant_index, tenant_slot_table):
    slot_ids = tenant_slot_table[sequence_tenant_index].astype(jnp.int32)
    sequence_input_rows = hidden.reshape(SEQS, LEN, MODEL_WIDTH)
    seq_grads = value_output_gradient.reshape(SEQS, LEN, VALUE_FEATURES)

    def per_sequence(seq_items):
        x_seq, g_seq, adapter_slot_index = seq_items
        chosen_down_factor = adapter_down_weight[adapter_slot_index]
        chosen_up_factor = adapter_up_weight[adapter_slot_index]
        reduced_rank_partial = jnp.dot(x_seq, chosen_down_factor, preferred_element_type=jnp.float32)
        adapter_output_term = jnp.dot(reduced_rank_partial, chosen_up_factor.astype(jnp.float32), precision=highest_precision)
        frozen_value_output = jnp.dot(x_seq, frozen_value_weight, preferred_element_type=jnp.float32)
        projected_values = (frozen_value_output + adapter_output_term).astype(jnp.bfloat16)
        backward_lowrank_term = jnp.dot(g_seq, chosen_up_factor.T, preferred_element_type=jnp.float32).astype(jnp.bfloat16)
        grad_in = jnp.dot(g_seq, frozen_value_weight.T, preferred_element_type=jnp.float32)
        grad_in = grad_in + jnp.dot(backward_lowrank_term, chosen_down_factor.T, preferred_element_type=jnp.float32)
        down_term = jnp.dot(x_seq.T, backward_lowrank_term, preferred_element_type=jnp.float32)
        up_term = jnp.dot(reduced_rank_partial.T, g_seq.astype(jnp.float32), precision=highest_precision)
        return projected_values, grad_in.astype(jnp.bfloat16), down_term, up_term

    projected_values, grad_in, down_terms, up_terms = lax.map(per_sequence, (sequence_input_rows, seq_grads, slot_ids))
    down_grad = jax.ops.segment_sum(down_terms, slot_ids, num_segments=TENANT_SLOTS)
    up_grad = jax.ops.segment_sum(up_terms, slot_ids, num_segments=TENANT_SLOTS)
    return (projected_values.reshape(TOKENS, VALUE_FEATURES), grad_in.reshape(TOKENS, MODEL_WIDTH), down_grad, up_grad)
```

```python
import jax
import jax.numpy as jnp
from jax import lax
from jax.sharding import PartitionSpec as P

HIGH = lax.Precision.HIGHEST
F32 = jnp.float32
BF16 = jnp.bfloat16


def inner_size(n):
    return max(q for q in range(1, n + 1) if n % q == 0 and q * q <= n)


def peer(i, d, n):
    return i ^ d if n & (n - 1) == 0 else (i + d) % n


def back(i, d, n):
    return i ^ d if n & (n - 1) == 0 else (i - d) % n


def offset(dst, src, n):
    return dst ^ src if n & (n - 1) == 0 else (dst - src) % n


def program(n, m):
    q = inner_size(n)
    r = n // q

    def send_inner(x, d):
        return lax.ppermute(x, "dp", [(i, i // q * q + peer(i % q, d, q)) for i in range(n)])

    def send_outer(x, d):
        return lax.ppermute(x, "dp", [(i, peer(i // q, d, r) * q + i % q) for i in range(n)])

    def swap(x):
        return lax.ppermute(x, "mp", [(0, 1), (1, 0)])

    def mp_sum(x):
        return x + swap(x) if m == 2 else lax.psum(x, "mp")

    def local(hidden, weight, down, up, grad, tenant, table):
        seqs = tenant.shape[0]
        rows, width = hidden.shape
        rank = down.shape[2]
        cols = grad.shape[1]
        length = rows // seqs
        me = lax.axis_index("dp")
        my_in, my_out = me % q, me // q
        core = lax.axis_index("mp")

        mine = jnp.concatenate([jnp.swapaxes(down[0], 0, 1), up[0]], axis=1)
        held = [mine] + [send_outer(mine, d) for d in range(1, r)]
        ids = table[tenant]
        near_ids = [ids] + [send_inner(ids, d) for d in range(1, q)]
        where_out = [offset(my_out, v // q, r) for v in near_ids]

        def pick(choice, parts):
            out = parts[0]
            for k in range(1, len(parts)):
                out = jnp.where(choice == k, parts[k], out)
            return out

        def wanted(d):
            o = d if q & (q - 1) == 0 else (q - d) % q
            return jnp.stack([pick(where_out[o][j], held) for j in range(seqs)])

        got = [wanted(0)] + [send_inner(wanted(d), d) for d in range(1, q)]
        from_in = offset(my_in, ids % q, q)
        chosen = jnp.stack([pick(from_in[j], [g[j] for g in got]) for j in range(seqs)])
        down_s, up_s = chosen[:, :, :width], chosen[:, :, width:]

        h3 = hidden.reshape(seqs, length, width)
        g3 = grad.reshape(seqs, length, cols)
        if m == 2:
            other = swap(grad)
            grad_full = jnp.where(core == 0, jnp.concatenate([grad, other], 1), jnp.concatenate([other, grad], 1))
        else:
            grad_full = lax.all_gather(grad, "mp", axis=1, tiled=True)
        base = jnp.dot(hidden, weight, preferred_element_type=F32)
        if m == 2:
            theirs = jnp.where(core == 0, base[:, cols:], base[:, :cols])
            ours = jnp.where(core == 0, base[:, :cols], base[:, cols:])
            base_own = ours + swap(theirs)
        else:
            base_own = lax.psum_scatter(base, "mp", scatter_dimension=1, tiled=True)

        back_low = mp_sum(jnp.einsum("slk,srk->srl", g3, up_s, preferred_element_type=F32)).astype(BF16)
        low = mp_sum(jnp.einsum("slw,srw->srl", h3, down_s, preferred_element_type=F32))
        up_f = up_s.astype(F32)
        values = (base_own.reshape(seqs, length, cols) + jnp.einsum("srl,srk->slk", low, up_f, precision=HIGH)).astype(BF16)
        up_seq = jnp.einsum("srl,slk->srk", low, g3.astype(F32), precision=HIGH)
        down_seq = jnp.einsum("srl,slw->srw", back_low, h3, preferred_element_type=F32)
        hidden_grad = (
            lax.dot_general(grad_full, weight, (((1,), (1,)), ((), ())), preferred_element_type=F32)
            + jnp.einsum("srl,srw->slw", back_low, down_s, preferred_element_type=F32).reshape(rows, width)
        ).astype(BF16)

        items = jnp.concatenate([down_seq, up_seq], axis=2)
        small = items.astype(BF16)
        near = [items] + [send_inner(small, d) for d in range(1, q)]
        totals = []
        for k in range(r):
            total = jnp.zeros((rank, width + cols), F32)
            for d in range(q):
                here = (near_ids[d] % q == my_in) & (where_out[d] == k)
                for j in range(seqs):
                    total = total + jnp.where(here[j], near[d][j].astype(F32), 0.0)
            totals.append(total)
        result = totals[0]
        for k in range(1, r):
            o = k if r & (r - 1) == 0 else (r - k) % r
            result = result + send_outer(totals[k].astype(BF16), o).astype(F32)
        down_grad = jnp.swapaxes(result[:, :width], 0, 1)[None]
        up_grad = result[None, :, width:]
        return values.reshape(rows, cols), hidden_grad, down_grad, up_grad

    return local


def solution(mesh):
    return jax.shard_map(
        program(mesh.shape["dp"], mesh.shape["mp"]),
        mesh=mesh,
        in_specs=(
            P("dp", "mp"),
            P("mp", None),
            P("dp", "mp", None),
            P("dp", None, "mp"),
            P("dp", "mp"),
            P("dp"),
            P(),
        ),
        out_specs=(P("dp", "mp"), P("dp", "mp"), P("dp", "mp", None), P("dp", None, "mp")),
        check_vma=False,
    )
```

```python
import jax
import jax.numpy as jnp
from jax import lax
from jax.experimental import pallas as pl
from jax.experimental.pallas import tpu as pltpu
from jax.sharding import PartitionSpec as P


HIGH = lax.Precision.HIGHEST
F32 = jnp.float32
BF16 = jnp.bfloat16


def inner_size(n):
    return max(q for q in range(1, n + 1) if n % q == 0 and q * q <= n)


def peer(i, d, n):
    return i ^ d if n & (n - 1) == 0 else (i + d) % n


def offset(dst, src, n):
    return dst ^ src if n & (n - 1) == 0 else (dst - src) % n


SMEM = pl.BlockSpec(memory_space=pltpu.SMEM)
VMEM = pl.BlockSpec(memory_space=pltpu.VMEM)
SMALL = pltpu.CompilerParams(vmem_limit_bytes=8 << 20)


def kernel_call(body, ints, arrays, outs, scratch=(), inside=True):
    arrays = [pltpu.with_memory_space_constraint(a, pltpu.VMEM) for a in arrays]
    return pl.pallas_call(
        body,
        out_shape=[pltpu.VMEM(o.shape, o.dtype) if inside else o for o in outs],
        in_specs=[SMEM] * len(ints) + [VMEM] * len(arrays),
        out_specs=[VMEM] * len(outs),
        scratch_shapes=list(scratch),
        compiler_params=SMALL,
    )(*ints, *arrays)


def program(n, m):
    q = inner_size(n)
    r = n // q

    def send_inner(x, d):
        return lax.ppermute(x, "dp", [(i, i // q * q + peer(i % q, d, q)) for i in range(n)])

    def send_outer(x, d):
        return lax.ppermute(x, "dp", [(i, peer(i // q, d, r) * q + i % q) for i in range(n)])

    def swap(x):
        return lax.ppermute(x, "mp", [(0, 1), (1, 0)])

    def mp_sum(x):
        return x + swap(x) if m == 2 else lax.psum(x, "mp")

    def opposite(d, size):
        return d if size & (size - 1) == 0 else (size - d) % size

    def local(hidden, weight, down, up, grad, tenant, table):
        seqs = tenant.shape[0]
        rows, width = hidden.shape
        rank = down.shape[2]
        cols = grad.shape[1]
        length = rows // seqs
        me = lax.axis_index("dp").astype(jnp.int32)[None]
        core = lax.axis_index("mp")

        def join(down_ref, up_ref, out):
            out[:, :width] = down_ref[...]
            out[:, width:] = up_ref[...]

        mine = pl.pallas_call(
            join, out_shape=pltpu.VMEM((rank, width + cols), BF16), compiler_params=SMALL, name="join"
        )(
            pltpu.with_memory_space_constraint(jnp.swapaxes(down[0], 0, 1), pltpu.HBM),
            pltpu.with_memory_space_constraint(up[0], pltpu.HBM),
        )
        held, tenants = [mine], [tenant]
        for d in range(1, r):
            held.append(send_outer(mine, d))
        for d in range(1, q):
            tenants.append(send_inner(tenant, d))
        ints = [me, table] + tenants

        def load(source, target, sem):
            pltpu.make_async_copy(source, target, sem).start()
            pltpu.make_async_copy(source, target, sem).wait()

        hidden = pl.pallas_call(
            load,
            out_shape=pltpu.VMEM(hidden.shape, BF16),
            in_specs=[pl.BlockSpec(memory_space=pl.ANY)],
            out_specs=VMEM,
            scratch_shapes=[pltpu.SemaphoreType.DMA(())],
            compiler_params=SMALL,
            name="load",
        )(hidden)

        def slot(refs, d, j):
            return refs[1][refs[2 + d][j]]

        def pick(*refs):
            ins, parts, outs = refs[: 2 + q], refs[2 + q : 2 + q + r], refs[2 + q + r :]
            outer = ins[0][0] // q
            for d in range(1, q):
                for j in range(seqs):
                    have = offset(outer, slot(ins, opposite(d, q), j) // q, r)
                    for k in range(r):

                        @pl.when(have == k)
                        def _(d=d, j=j, k=k):
                            outs[d - 1][j] = parts[k][...]

        sent = kernel_call(pick, ints, held, [jax.ShapeDtypeStruct((seqs, rank, width + cols), BF16)] * (q - 1))
        got = []
        for d in range(1, q):
            got.append(send_inner(sent[d - 1], d))

        def choose(*refs):
            ins, parts = refs[: 2 + q], refs[2 + q : 2 + q + r]
            gots, (down_out, up_out) = refs[2 + q + r : 1 + 2 * q + r], refs[1 + 2 * q + r :]
            inner, outer = ins[0][0] % q, ins[0][0] // q
            for j in range(seqs):
                wanted = slot(ins, 0, j)
                way = offset(inner, wanted % q, q)
                have = offset(outer, wanted // q, r)
                for d in range(1, q):

                    @pl.when(way == d)
                    def _(d=d, j=j):
                        down_out[j] = gots[d - 1][j, :, :width]
                        up_out[j] = gots[d - 1][j, :, width:]

                for k in range(r):

                    @pl.when((way == 0) & (have == k))
                    def _(j=j, k=k):
                        down_out[j] = parts[k][:, :width]
                        up_out[j] = parts[k][:, width:]

        down_s, up_s = kernel_call(
            choose,
            ints,
            held + got,
            [jax.ShapeDtypeStruct((seqs, rank, width), BF16), jax.ShapeDtypeStruct((seqs, rank, cols), BF16)],
        )

        h3 = hidden.reshape(seqs, length, width)
        g3 = grad.reshape(seqs, length, cols)
        if m == 2:
            other = swap(grad)
            grad_full = jnp.where(core == 0, jnp.concatenate([grad, other], 1), jnp.concatenate([other, grad], 1))
        else:
            grad_full = lax.all_gather(grad, "mp", axis=1, tiled=True)
        base = jnp.dot(hidden, weight, preferred_element_type=F32)
        if m == 2:
            theirs = jnp.where(core == 0, base[:, cols:], base[:, :cols])
            ours = jnp.where(core == 0, base[:, :cols], base[:, cols:])
            base_got = swap(theirs)
            base_own = ours + base_got
        else:
            base_own = lax.psum_scatter(base, "mp", scatter_dimension=1, tiled=True)

        back_low = mp_sum(jnp.einsum("slk,srk->srl", g3, up_s, preferred_element_type=F32)).astype(BF16)
        low = mp_sum(jnp.einsum("slw,srw->srl", h3, down_s, preferred_element_type=F32))
        up_f = up_s.astype(F32)
        values = (base_own.reshape(seqs, length, cols) + jnp.einsum("srl,srk->slk", low, up_f, precision=HIGH)).astype(BF16)
        up_seq = jnp.einsum("srl,slk->srk", low, g3.astype(F32), precision=HIGH)
        down_seq = jnp.einsum("srl,slw->srw", back_low, h3, preferred_element_type=F32)
        hidden_grad = (
            lax.dot_general(grad_full, weight, (((1,), (1,)), ((), ())), preferred_element_type=F32)
            + jnp.einsum("srl,srw->slw", back_low, down_s, preferred_element_type=F32).reshape(rows, width)
        ).astype(BF16)

        items = jnp.concatenate([down_seq, up_seq], axis=2)
        small = items.astype(BF16)
        near = []
        for d in range(1, q):
            near.append(send_inner(small, d))

        def gather_items(*refs):
            ins, own, others = refs[: 2 + q], refs[2 + q], refs[3 + q : 2 + 2 * q]
            outs, acc = refs[2 + 2 * q : -1], refs[-1]
            inner, outer = ins[0][0] % q, ins[0][0] // q
            acc[...] = jnp.zeros_like(acc)
            for d in range(q):
                for j in range(seqs):
                    holder = slot(ins, d, j)

                    @pl.when(holder % q == inner)
                    def _(d=d, j=j, holder=holder):
                        k = offset(outer, holder // q, r)
                        item = own[j] if d == 0 else others[d - 1][j].astype(F32)
                        acc[k] += item

            outs[0][...] = acc[0]
            for k in range(1, r):
                outs[k][...] = acc[k].astype(BF16)

        shape = (rank, width + cols)
        totals = kernel_call(
            gather_items,
            ints,
            [items] + near,
            [jax.ShapeDtypeStruct(shape, F32)] + [jax.ShapeDtypeStruct(shape, BF16)] * (r - 1),
            [pltpu.VMEM((r,) + shape, F32)],
        )
        arrived = []
        for k in range(1, r):
            arrived.append(send_outer(totals[k], opposite(k, r)))
        values, hidden_grad, arrived = lax.optimization_barrier((values, hidden_grad, arrived))

        def finish(*refs):
            own, others, down_out, up_out = refs[0], refs[1:r], refs[r], refs[r + 1]
            total = own[...]
            for other in others:
                total = total + other[...].astype(F32)
            down_out[...] = total[:, :width]
            up_out[...] = total[:, width:]

        down_grad, up_grad = kernel_call(
            finish,
            [],
            [totals[0]] + arrived,
            [jax.ShapeDtypeStruct((rank, width), F32), jax.ShapeDtypeStruct((rank, cols), F32)],
            inside=False,
        )
        down_grad = jnp.swapaxes(down_grad, 0, 1)[None]
        return values.reshape(rows, cols), hidden_grad, down_grad, up_grad[None]

    return local


def solution(mesh):
    n, m = mesh.shape["dp"], mesh.shape["mp"]
    return jax.shard_map(
        program(n, m),
        mesh=mesh,
        in_specs=(
            P("dp", "mp"),
            P("mp", None),
            P("dp", "mp", None),
            P("dp", None, "mp"),
            P("dp", "mp"),
            P("dp"),
            P(),
        ),
        out_specs=(P("dp", "mp"), P("dp", "mp"), P("dp", "mp", None), P("dp", None, "mp")),
        check_vma=False,
    )
```

```python
import math

import jax
import jax.numpy as jnp
from jax import lax
from jax.experimental import pallas as pl
from jax.experimental.pallas import tpu as pltpu
from jax.sharding import PartitionSpec as P


HIGH = lax.Precision.HIGHEST
F32 = jnp.float32
BF16 = jnp.bfloat16


def inner_size(n):
    return max(q for q in range(1, n + 1) if n % q == 0 and q * q <= n)


def peer(i, d, n):
    return i ^ d if n & (n - 1) == 0 else (i + d) % n


def offset(dst, src, n):
    return dst ^ src if n & (n - 1) == 0 else (dst - src) % n


SMEM = pl.BlockSpec(memory_space=pltpu.SMEM)
VMEM = pl.BlockSpec(memory_space=pltpu.VMEM)
SMALL = pltpu.CompilerParams(vmem_limit_bytes=8 << 20)


def fixed(x):
    return pltpu.with_memory_space_constraint(x, pltpu.HBM)


def kernel_call(body, ints, arrays, outs, scratch=(), inside=True):
    arrays = [pltpu.with_memory_space_constraint(a, pltpu.VMEM) for a in arrays]
    return pl.pallas_call(
        body,
        out_shape=[pltpu.VMEM(o.shape, o.dtype) if inside else o for o in outs],
        in_specs=[SMEM] * len(ints) + [VMEM] * len(arrays),
        out_specs=[VMEM] * len(outs),
        scratch_shapes=list(scratch),
        compiler_params=SMALL,
    )(*ints, *arrays)


def program(n, m):
    q = inner_size(n)
    r = n // q

    def send_inner(x, d):
        return lax.ppermute(x, "dp", [(i, i // q * q + peer(i % q, d, q)) for i in range(n)])

    def send_outer(x, d):
        return lax.ppermute(x, "dp", [(i, peer(i // q, d, r) * q + i % q) for i in range(n)])

    def swap(x):
        return lax.ppermute(x, "mp", [(0, 1), (1, 0)])

    def mp_sum(x):
        return x + swap(x) if m == 2 else lax.psum(x, "mp")

    def opposite(d, size):
        return d if size & (size - 1) == 0 else (size - d) % size

    def local(hidden, weight, down, up, grad, tenant, table):
        seqs = tenant.shape[0]
        rows, width = hidden.shape
        rank = down.shape[2]
        cols = grad.shape[1]
        length = rows // seqs
        block = math.gcd(length, 384)
        me = lax.axis_index("dp").astype(jnp.int32)[None]
        core = lax.axis_index("mp").astype(jnp.int32)[None]
        low_core = lax.axis_index("mp") == 0
        me, core, low_core, down, up, tenant = lax.optimization_barrier((me, core, low_core, down, up, tenant))

        first = max(width - cols, 256) // 256 * 128
        rest = width - first

        def join(down_ref, up_ref, out0, out1):
            out0[:, :first] = down_ref[:, :first]
            out0[:, first:] = up_ref[...]
            out1[...] = down_ref[:, first:]

        mine = pl.pallas_call(
            join,
            out_shape=[pltpu.VMEM((rank, first + cols), BF16), pltpu.VMEM((rank, rest), BF16)],
            compiler_params=SMALL,
            name="join",
        )(
            fixed(jnp.swapaxes(down[0], 0, 1)),
            fixed(up[0]),
        )
        held, tenants = [[mine[0]], [mine[1]]], [tenant]
        for p in range(2):
            for d in range(1, r):
                held[p].append(send_outer(mine[p], d))
        for d in range(1, q):
            tenants.append(send_inner(tenant, d))
        ints = [me, fixed(table), fixed(tenant)] + tenants[1:]

        def load(x_ref, g_ref, x_out, g_out, sems):
            copies = [
                pltpu.make_async_copy(x_ref, x_out, sems.at[0]),
                pltpu.make_async_copy(g_ref, g_out, sems.at[1]),
            ]
            for c in copies:
                c.start()
            for c in copies:
                c.wait()

        hidden, grad_in = pl.pallas_call(
            load,
            out_shape=[pltpu.VMEM(hidden.shape, BF16), pltpu.VMEM(grad.shape, BF16)],
            in_specs=[pl.BlockSpec(memory_space=pl.ANY)] * 2,
            out_specs=[VMEM] * 2,
            scratch_shapes=[pltpu.SemaphoreType.DMA((2,))],
            compiler_params=SMALL,
            name="load",
        )(fixed(hidden), fixed(grad))

        def slot(refs, d, j):
            return refs[1][refs[2 + d][j]]

        def pick(*refs):
            ins, parts, outs = refs[: 2 + q], refs[2 + q : 2 + q + r], refs[2 + q + r :]
            outer = ins[0][0] // q
            for d in range(1, q):
                for j in range(seqs):
                    have = offset(outer, slot(ins, opposite(d, q), j) // q, r)
                    for k in range(r):

                        @pl.when(have == k)
                        def _(d=d, j=j, k=k):
                            outs[d - 1][j] = parts[k][...]

        got = []
        for p in range(2):
            sent = kernel_call(pick, ints, held[p], [jax.ShapeDtypeStruct((seqs,) + held[p][0].shape, BF16)] * (q - 1))
            got.append([])
            for d in range(1, q):
                got[p].append(send_inner(sent[d - 1], d))

        def chosen(refs, store):
            ins, parts, gots = refs[: 2 + q], refs[2 + q : 2 + q + r], refs[2 + q + r : 1 + 2 * q + r]
            inner, outer = ins[0][0] % q, ins[0][0] // q
            for j in range(seqs):
                wanted = slot(ins, 0, j)
                way = offset(inner, wanted % q, q)
                have = offset(outer, wanted // q, r)
                for d in range(1, q):

                    @pl.when(way == d)
                    def _(d=d, j=j):
                        store(j, gots[d - 1].at[j])

                for k in range(r):

                    @pl.when((way == 0) & (have == k))
                    def _(j=j, k=k):
                        store(j, parts[k])

        def choose0(*refs):
            down_out, up_out = refs[-2:]

            def store(j, ref):
                down_out[j] = ref[:, :first]
                up_out[j] = ref[:, first:]

            chosen(refs, store)

        def choose1(*refs):
            down_in, down_out = refs[-2:]
            down_out[:, :, :first] = down_in[...]

            def store(j, ref):
                down_out[j, :, first:] = ref[...]

            chosen(refs, store)

        down_first, up_s = kernel_call(
            choose0,
            ints,
            held[0] + got[0],
            [jax.ShapeDtypeStruct((seqs, rank, first), BF16), jax.ShapeDtypeStruct((seqs, rank, cols), BF16)],
        )
        (down_s,) = kernel_call(
            choose1, ints, held[1] + got[1] + [down_first], [jax.ShapeDtypeStruct((seqs, rank, width), BF16)]
        )

        h3 = hidden.reshape(seqs, length, width)
        g3 = grad_in.reshape(seqs, length, cols)
        if m == 2:
            other = swap(grad_in)
        else:
            grad_full = lax.all_gather(grad, "mp", axis=1, tiled=True)
        base = []
        for j in range(seqs):
            base.append(jnp.dot(h3[j], weight, preferred_element_type=F32))
        base = jnp.concatenate(base)
        if m == 2:
            theirs = jnp.where(low_core, base[:, cols:], base[:, :cols])
            ours = jnp.where(low_core, base[:, :cols], base[:, cols:])
            base_got = swap(theirs)
            base_own = ours + base_got
        else:
            base_own = lax.psum_scatter(base, "mp", scatter_dimension=1, tiled=True)

        back_low = mp_sum(jnp.einsum("slk,srk->srl", g3, up_s, preferred_element_type=F32)).astype(BF16)
        low = mp_sum(jnp.einsum("slw,srw->srl", h3, down_s, preferred_element_type=F32))
        up_f = up_s.astype(F32)
        values = (base_own.reshape(seqs, length, cols) + jnp.einsum("srl,srk->slk", low, up_f, precision=HIGH)).astype(BF16)
        up_seq = jnp.einsum("srl,slk->srk", low, g3.astype(F32), precision=HIGH)
        down_seq = jnp.einsum("srl,slw->srw", back_low, h3, preferred_element_type=F32)
        if m == 2:
            per = length // block

            def widen(core_ref, own, mate, w, coeff, factor, out):
                def part(x, half):
                    at = pl.multiple_of(half * cols, math.gcd(cols, 128))
                    return lax.dot_general(
                        x[...], w[:, pl.ds(at, cols)], (((1,), (1,)), ((), ())), preferred_element_type=F32
                    )

                total = part(own, core_ref[0]) + part(mate, 1 - core_ref[0])
                total += lax.dot_general(
                    coeff[0], factor[0], (((0,), (0,)), ((), ())), preferred_element_type=F32
                )
                out[...] = total.astype(BF16)

            rows_of = pl.BlockSpec((block, cols), lambda i: (i, 0))
            hidden_grad = pl.pallas_call(
                widen,
                grid=(rows // block,),
                out_shape=jax.ShapeDtypeStruct((rows, width), BF16),
                in_specs=[
                    SMEM,
                    rows_of,
                    rows_of,
                    pl.BlockSpec((width, m * cols), lambda i: (0, 0)),
                    pl.BlockSpec((1, rank, block), lambda i: (i // per, 0, i % per)),
                    pl.BlockSpec((1, rank, width), lambda i: (i // per, 0, 0)),
                ],
                out_specs=pl.BlockSpec((block, width), lambda i: (i, 0)),
                compiler_params=pltpu.CompilerParams(vmem_limit_bytes=24 << 20),
                name="widen",
            )(core, grad_in, other, weight, back_low, down_s)
        else:
            hidden_grad = (
                lax.dot_general(grad_full, weight, (((1,), (1,)), ((), ())), preferred_element_type=F32)
                + jnp.einsum("srl,srw->slw", back_low, down_s, preferred_element_type=F32).reshape(rows, width)
            ).astype(BF16)

        items = [down_seq[:, :, :rest], jnp.concatenate([down_seq[:, :, rest:], up_seq], axis=2)]
        near = [[], []]
        for p in range(2):
            small = items[p].astype(BF16)
            for d in range(1, q):
                near[p].append(send_inner(small, d))

        def gather_items(*refs):
            ins, own, others = refs[: 2 + q], refs[2 + q : 4 + q], refs[4 + q : 2 + 3 * q]
            outs, acc = refs[2 + 3 * q : -1], refs[-1]
            inner, outer = ins[0][0] % q, ins[0][0] // q
            acc[...] = jnp.zeros_like(acc)
            for d in range(q):
                for j in range(seqs):
                    holder = slot(ins, d, j)

                    @pl.when(holder % q == inner)
                    def _(d=d, j=j, holder=holder):
                        k = offset(outer, holder // q, r)
                        for p, at in ((0, slice(0, rest)), (1, slice(rest, None))):
                            piece = own[p] if d == 0 else others[p * (q - 1) + d - 1]
                            acc[k, :, at] += piece[j].astype(F32)

            outs[0][...] = acc[0]
            for k in range(1, r):
                outs[k][...] = acc[k].astype(BF16)

        shape = (rank, width + cols)
        parts = kernel_call(
            gather_items,
            ints,
            items + near[0] + near[1],
            [jax.ShapeDtypeStruct(shape, F32)] + [jax.ShapeDtypeStruct(shape, BF16)] * (r - 1),
            [pltpu.VMEM((r,) + shape, F32)],
        )
        arrived = []
        for k in range(1, r):
            arrived.append(send_outer(parts[k], opposite(k, r)))
        values, hidden_grad, arrived = lax.optimization_barrier((values, hidden_grad, arrived))

        def finish(*refs):
            others, down_out, up_out = refs[:r], refs[r], refs[r + 1]
            total = others[0][...]
            for other in others[1:]:
                total = total + other[...].astype(F32)
            down_out[...] = total[:, :width]
            up_out[...] = total[:, width:]

        down_grad, up_grad = kernel_call(
            finish,
            [],
            [parts[0]] + arrived,
            [jax.ShapeDtypeStruct((rank, width), F32), jax.ShapeDtypeStruct((rank, cols), F32)],
            inside=False,
        )
        down_grad = jnp.swapaxes(down_grad, 0, 1)[None]
        return values.reshape(rows, cols), hidden_grad, down_grad, up_grad[None]

    return local


def solution(mesh):
    n, m = mesh.shape["dp"], mesh.shape["mp"]
    return jax.shard_map(
        program(n, m),
        mesh=mesh,
        in_specs=(
            P("dp", "mp"),
            P("mp", None),
            P("dp", "mp", None),
            P("dp", None, "mp"),
            P("dp", "mp"),
            P("dp"),
            P(),
        ),
        out_specs=(P("dp", "mp"), P("dp", "mp"), P("dp", "mp", None), P("dp", None, "mp")),
        check_vma=False,
    )
```

```python
import math

import jax
import jax.numpy as jnp
from jax import lax
from jax.experimental import pallas as pl
from jax.experimental.pallas import tpu as pltpu
from jax.sharding import PartitionSpec as P


HIGH = lax.Precision.HIGHEST
F32 = jnp.float32
BF16 = jnp.bfloat16


def inner_size(n):
    return max(q for q in range(1, n + 1) if n % q == 0 and q * q <= n)


def peer(i, d, n):
    return i ^ d if n & (n - 1) == 0 else (i + d) % n


def offset(dst, src, n):
    return dst ^ src if n & (n - 1) == 0 else (dst - src) % n


SMEM = pl.BlockSpec(memory_space=pltpu.SMEM)
VMEM = pl.BlockSpec(memory_space=pltpu.VMEM)
SMALL = pltpu.CompilerParams(vmem_limit_bytes=8 << 20)


def fixed(x):
    return pltpu.with_memory_space_constraint(x, pltpu.HBM)


def kernel_call(body, ints, arrays, outs, scratch=(), inside=True):
    arrays = [pltpu.with_memory_space_constraint(a, pltpu.VMEM) for a in arrays]
    return pl.pallas_call(
        body,
        out_shape=[pltpu.VMEM(o.shape, o.dtype) if inside else o for o in outs],
        in_specs=[SMEM] * len(ints) + [VMEM] * len(arrays),
        out_specs=[VMEM] * len(outs),
        scratch_shapes=list(scratch),
        compiler_params=SMALL,
    )(*ints, *arrays)


def program(n, m):
    q = inner_size(n)
    r = n // q

    def send_inner(x, d):
        return lax.ppermute(x, "dp", [(i, i // q * q + peer(i % q, d, q)) for i in range(n)])

    def send_outer(x, d):
        return lax.ppermute(x, "dp", [(i, peer(i // q, d, r) * q + i % q) for i in range(n)])

    def swap(x):
        return lax.ppermute(x, "mp", [(0, 1), (1, 0)])

    def mp_sum(x):
        return x + swap(x) if m == 2 else lax.psum(x, "mp")

    def opposite(d, size):
        return d if size & (size - 1) == 0 else (size - d) % size

    def local(hidden, weight, down, up, grad, tenant, table):
        seqs = tenant.shape[0]
        rows, width = hidden.shape
        rank = down.shape[2]
        cols = grad.shape[1]
        length = rows // seqs
        block = math.gcd(length, 384)
        me = lax.axis_index("dp").astype(jnp.int32)[None]
        core = lax.axis_index("mp").astype(jnp.int32)[None]
        low_core = lax.axis_index("mp") == 0
        me, core, low_core, down, up, tenant = lax.optimization_barrier((me, core, low_core, down, up, tenant))

        first = max(width * 768 // 1792 // 128 * 128, 128)
        rest = width - first

        def join(down_ref, up_ref, out0, out1):
            out0[:, :first] = down_ref[:, :first]
            out0[:, first:] = up_ref[...]
            out1[...] = down_ref[:, first:]

        mine = pl.pallas_call(
            join,
            out_shape=[pltpu.VMEM((rank, first + cols), BF16), pltpu.VMEM((rank, rest), BF16)],
            compiler_params=SMALL,
            name="join",
        )(
            fixed(jnp.swapaxes(down[0], 0, 1)),
            fixed(up[0]),
        )
        held, tenants = [[mine[0]], [mine[1]]], [tenant]
        for p in range(2):
            for d in range(1, r):
                held[p].append(send_outer(mine[p], d))
        for d in range(1, q):
            tenants.append(send_inner(tenant, d))
        ints = [me, fixed(table), fixed(tenant)] + tenants[1:]

        def load(x_ref, g_ref, x_out, g_out, sems):
            copies = [
                pltpu.make_async_copy(x_ref, x_out, sems.at[0]),
                pltpu.make_async_copy(g_ref, g_out, sems.at[1]),
            ]
            for c in copies:
                c.start()
            for c in copies:
                c.wait()

        hidden, grad_in = pl.pallas_call(
            load,
            out_shape=[pltpu.VMEM(hidden.shape, BF16), pltpu.VMEM(grad.shape, BF16)],
            in_specs=[pl.BlockSpec(memory_space=pl.ANY)] * 2,
            out_specs=[VMEM] * 2,
            scratch_shapes=[pltpu.SemaphoreType.DMA((2,))],
            compiler_params=SMALL,
            name="load",
        )(fixed(hidden), fixed(grad))

        def slot(refs, d, j):
            return refs[1][refs[2 + d][j]]

        def pick(*refs):
            ins, parts, outs = refs[: 2 + q], refs[2 + q : 2 + q + r], refs[2 + q + r :]
            outer = ins[0][0] // q
            for d in range(1, q):
                for j in range(seqs):
                    have = offset(outer, slot(ins, opposite(d, q), j) // q, r)
                    for k in range(r):

                        @pl.when(have == k)
                        def _(d=d, j=j, k=k):
                            outs[d - 1][j] = parts[k][...]

        got = []
        for p in range(2):
            sent = kernel_call(pick, ints, held[p], [jax.ShapeDtypeStruct((seqs,) + held[p][0].shape, BF16)] * (q - 1))
            got.append([])
            for d in range(1, q):
                got[p].append(send_inner(sent[d - 1], d))

        def chosen(refs, store):
            ins, parts, gots = refs[: 2 + q], refs[2 + q : 2 + q + r], refs[2 + q + r : 1 + 2 * q + r]
            inner, outer = ins[0][0] % q, ins[0][0] // q
            for j in range(seqs):
                wanted = slot(ins, 0, j)
                way = offset(inner, wanted % q, q)
                have = offset(outer, wanted // q, r)
                for d in range(1, q):

                    @pl.when(way == d)
                    def _(d=d, j=j):
                        store(j, gots[d - 1].at[j])

                for k in range(r):

                    @pl.when((way == 0) & (have == k))
                    def _(j=j, k=k):
                        store(j, parts[k])

        def choose0(*refs):
            down_out, up_out = refs[-2:]

            def store(j, ref):
                down_out[j] = ref[:, :first]
                up_out[j] = ref[:, first:]

            chosen(refs, store)

        def choose1(*refs):
            down_in, down_out = refs[-2:]
            down_out[:, :, :first] = down_in[...]

            def store(j, ref):
                down_out[j, :, first:] = ref[...]

            chosen(refs, store)

        down_first, up_s = kernel_call(
            choose0,
            ints,
            held[0] + got[0],
            [jax.ShapeDtypeStruct((seqs, rank, first), BF16), jax.ShapeDtypeStruct((seqs, rank, cols), BF16)],
        )
        (down_s,) = kernel_call(
            choose1, ints, held[1] + got[1] + [down_first], [jax.ShapeDtypeStruct((seqs, rank, width), BF16)]
        )

        h3 = hidden.reshape(seqs, length, width)
        g3 = grad_in.reshape(seqs, length, cols)
        if m == 2:
            other = swap(grad_in)
        else:
            grad_full = lax.all_gather(grad, "mp", axis=1, tiled=True)
        base = []
        for j in range(seqs):
            base.append(jnp.dot(h3[j], weight, preferred_element_type=F32))
        if m == 2:
            theirs = jnp.concatenate([jnp.where(low_core, x[:, cols:], x[:, :cols]) for x in base])
            base_got = swap(theirs)
        else:
            base_own = lax.psum_scatter(jnp.concatenate(base), "mp", scatter_dimension=1, tiled=True)

        back_low = mp_sum(jnp.einsum("slk,srk->srl", g3, up_s, preferred_element_type=F32)).astype(BF16)
        low = mp_sum(jnp.einsum("slw,srw->srl", h3, down_s, preferred_element_type=F32))
        up_seq = jnp.einsum("srl,slk->srk", low, g3.astype(F32), precision=HIGH)
        down_seq = jnp.einsum("srl,slw->srw", back_low, h3, preferred_element_type=F32)
        if m == 2:
            per = length // block

            def outputs(core_ref, own, mate, w, coeff, factor, low_ref, up_ref, got_ref, *rest_refs):
                bases, (out, values_out, lhs) = rest_refs[:seqs], rest_refs[seqs:]
                step = pl.program_id(0)
                here = pl.multiple_of(core_ref[0] * cols, math.gcd(cols, 128))
                there = pl.multiple_of((1 - core_ref[0]) * cols, math.gcd(cols, 128))
                lhs[:, pl.ds(here, cols)] = own[...]
                lhs[:, pl.ds(there, cols)] = mate[...]
                total = lax.dot_general(
                    lhs[...], w[...], (((1,), (1,)), ((), ())), preferred_element_type=F32
                ) + lax.dot_general(
                    coeff[0], factor[0], (((0,), (0,)), ((), ())), preferred_element_type=F32
                )
                out[...] = total.astype(BF16)
                term = got_ref[...] + lax.dot_general(
                    low_ref[0],
                    up_ref[0].astype(F32),
                    (((0,), (0,)), ((), ())),
                    precision=HIGH,
                    preferred_element_type=F32,
                )
                for j in range(seqs):

                    @pl.when(step // per == j)
                    def _(j=j):
                        at = pl.multiple_of(step % per * block, block)
                        values_out[...] = (term + bases[j][pl.ds(at, block), pl.ds(here, cols)]).astype(BF16)

            rows_of = pl.BlockSpec((block, cols), lambda i: (i, 0))
            coeff_of = pl.BlockSpec((1, rank, block), lambda i: (i // per, 0, i % per))
            values, hidden_grad = pl.pallas_call(
                outputs,
                grid=(rows // block,),
                out_shape=[
                    jax.ShapeDtypeStruct((rows, width), BF16),
                    jax.ShapeDtypeStruct((rows, cols), BF16),
                ],
                in_specs=[
                    SMEM,
                    rows_of,
                    rows_of,
                    VMEM,
                    coeff_of,
                    pl.BlockSpec((1, rank, width), lambda i: (i // per, 0, 0)),
                    coeff_of,
                    pl.BlockSpec((1, rank, cols), lambda i: (i // per, 0, 0)),
                    rows_of,
                ]
                + [VMEM] * seqs,
                out_specs=[pl.BlockSpec((block, width), lambda i: (i, 0)), rows_of],
                scratch_shapes=[pltpu.VMEM((block, m * cols), BF16)],
                compiler_params=pltpu.CompilerParams(vmem_limit_bytes=24 << 20),
                name="outputs",
            )(core, grad_in, other, weight, back_low, down_s, low, up_s, base_got, *base)[::-1]
        else:
            values = (
                base_own.reshape(seqs, length, cols)
                + jnp.einsum("srl,srk->slk", low, up_s.astype(F32), precision=HIGH)
            ).astype(BF16)
            hidden_grad = (
                lax.dot_general(grad_full, weight, (((1,), (1,)), ((), ())), preferred_element_type=F32)
                + jnp.einsum("srl,srw->slw", back_low, down_s, preferred_element_type=F32).reshape(rows, width)
            ).astype(BF16)

        items = [down_seq, up_seq]
        near = [[], []]
        for p in range(2):
            small = items[p].astype(BF16)
            for d in range(1, q):
                near[p].append(send_inner(small, d))

        def gather_items(*refs):
            ins, own, others = refs[: 2 + q], refs[2 + q : 4 + q], refs[4 + q : 2 + 3 * q]
            outs, acc = refs[2 + 3 * q : -1], refs[-1]
            inner, outer = ins[0][0] % q, ins[0][0] // q
            acc[...] = jnp.zeros_like(acc)
            for d in range(q):
                for j in range(seqs):
                    holder = slot(ins, d, j)

                    @pl.when(holder % q == inner)
                    def _(d=d, j=j, holder=holder):
                        k = offset(outer, holder // q, r)
                        for p, at in ((0, slice(0, width)), (1, slice(width, None))):
                            piece = own[p] if d == 0 else others[p * (q - 1) + d - 1]
                            acc[k, :, at] += piece[j].astype(F32)

            outs[0][...] = acc[0]
            for k in range(1, r):
                outs[k][...] = acc[k].astype(BF16)

        shape = (rank, width + cols)
        parts = kernel_call(
            gather_items,
            ints,
            items + near[0] + near[1],
            [jax.ShapeDtypeStruct(shape, F32)] + [jax.ShapeDtypeStruct(shape, BF16)] * (r - 1),
            [pltpu.VMEM((r,) + shape, F32)],
        )
        arrived = []
        for k in range(1, r):
            arrived.append(send_outer(parts[k], opposite(k, r)))
        values, hidden_grad, arrived = lax.optimization_barrier((values, hidden_grad, arrived))

        def finish(*refs):
            others, down_out, up_out = refs[:r], refs[r], refs[r + 1]
            total = others[0][...]
            for other in others[1:]:
                total = total + other[...].astype(F32)
            down_out[...] = total[:, :width]
            up_out[...] = total[:, width:]

        down_grad, up_grad = kernel_call(
            finish,
            [],
            [parts[0]] + arrived,
            [jax.ShapeDtypeStruct((rank, width), F32), jax.ShapeDtypeStruct((rank, cols), F32)],
            inside=False,
        )
        down_grad = jnp.swapaxes(down_grad, 0, 1)[None]
        return values.reshape(rows, cols), hidden_grad, down_grad, up_grad[None]

    return local


def solution(mesh):
    n, m = mesh.shape["dp"], mesh.shape["mp"]
    return jax.shard_map(
        program(n, m),
        mesh=mesh,
        in_specs=(
            P("dp", "mp"),
            P("mp", None),
            P("dp", "mp", None),
            P("dp", None, "mp"),
            P("dp", "mp"),
            P("dp"),
            P(),
        ),
        out_specs=(P("dp", "mp"), P("dp", "mp"), P("dp", "mp", None), P("dp", None, "mp")),
        check_vma=False,
    )
```

```python
import math

import jax
import jax.numpy as jnp
from jax import lax
from jax.experimental import pallas as pl
from jax.experimental.pallas import tpu as pltpu
from jax.sharding import PartitionSpec as P


HIGH = lax.Precision.HIGHEST
F32 = jnp.float32
BF16 = jnp.bfloat16


def inner_size(n):
    return max(q for q in range(1, n + 1) if n % q == 0 and q * q <= n)


def peer(i, d, n):
    return i ^ d if n & (n - 1) == 0 else (i + d) % n


def offset(dst, src, n):
    return dst ^ src if n & (n - 1) == 0 else (dst - src) % n


SMEM = pl.BlockSpec(memory_space=pltpu.SMEM)
VMEM = pl.BlockSpec(memory_space=pltpu.VMEM)
SMALL = pltpu.CompilerParams(vmem_limit_bytes=8 << 20)


def fixed(x):
    return pltpu.with_memory_space_constraint(x, pltpu.HBM)


def kernel_call(body, ints, arrays, outs, scratch=(), inside=True):
    arrays = [pltpu.with_memory_space_constraint(a, pltpu.VMEM) for a in arrays]
    return pl.pallas_call(
        body,
        out_shape=[pltpu.VMEM(o.shape, o.dtype) if inside else o for o in outs],
        in_specs=[SMEM] * len(ints) + [VMEM] * len(arrays),
        out_specs=[VMEM] * len(outs),
        scratch_shapes=list(scratch),
        compiler_params=SMALL,
    )(*ints, *arrays)


def program(n, m):
    q = inner_size(n)
    r = n // q

    def send_inner(x, d):
        return lax.ppermute(x, "dp", [(i, i // q * q + peer(i % q, d, q)) for i in range(n)])

    def send_outer(x, d):
        return lax.ppermute(x, "dp", [(i, peer(i // q, d, r) * q + i % q) for i in range(n)])

    def swap(x):
        return lax.ppermute(x, "mp", [(0, 1), (1, 0)])

    def mp_sum(x):
        return x + swap(x) if m == 2 else lax.psum(x, "mp")

    def opposite(d, size):
        return d if size & (size - 1) == 0 else (size - d) % size

    def local(hidden, weight, down, up, grad, tenant, table):
        seqs = tenant.shape[0]
        rows, width = hidden.shape
        rank = down.shape[2]
        cols = grad.shape[1]
        length = rows // seqs
        block = math.gcd(length, 768)
        me = lax.axis_index("dp").astype(jnp.int32)[None]
        core = lax.axis_index("mp").astype(jnp.int32)[None]
        low_core = lax.axis_index("mp") == 0
        me, core, low_core, down, up, tenant = lax.optimization_barrier((me, core, low_core, down, up, tenant))

        first = max(width * 512 // 1792 // 128 * 128, 128)
        rest = width - first

        def join(down_ref, up_ref, out):
            out[:, :width] = down_ref[...]
            out[:, width:] = up_ref[...]

        mine = pl.pallas_call(
            join,
            out_shape=pltpu.VMEM((rank, width + cols), BF16),
            compiler_params=SMALL,
            name="join",
        )(fixed(jnp.swapaxes(down[0], 0, 1)), fixed(up[0]))
        held, tenants = [mine], [tenant]
        for d in range(1, r):
            held.append(send_outer(mine, d))
        for d in range(1, q):
            tenants.append(send_inner(tenant, d))
        ints = [me, fixed(table), fixed(tenant)] + tenants[1:]

        def load(x_ref, g_ref, x_out, g_out, sems):
            copies = [
                pltpu.make_async_copy(x_ref, x_out, sems.at[0]),
                pltpu.make_async_copy(g_ref, g_out, sems.at[1]),
            ]
            for c in copies:
                c.start()
            for c in copies:
                c.wait()

        hidden, grad_in = pl.pallas_call(
            load,
            out_shape=[pltpu.VMEM(hidden.shape, BF16), pltpu.VMEM(grad.shape, BF16)],
            in_specs=[pl.BlockSpec(memory_space=pl.ANY)] * 2,
            out_specs=[VMEM] * 2,
            scratch_shapes=[pltpu.SemaphoreType.DMA((2,))],
            compiler_params=SMALL,
            name="load",
        )(fixed(hidden), fixed(grad))

        def slot(refs, d, j):
            return refs[1][refs[2 + d][j]]

        def pick(*refs):
            ins, parts, outs = refs[: 2 + q], refs[2 + q : 2 + q + r], refs[2 + q + r :]
            outer = ins[0][0] // q
            for d in range(1, q):
                for j in range(seqs):
                    have = offset(outer, slot(ins, opposite(d, q), j) // q, r)
                    for k in range(r):

                        @pl.when(have == k)
                        def _(d=d, j=j, k=k):
                            outs[d - 1][j, :, :first] = parts[k][:, :first]
                            outs[d - 1][j, :, first:] = parts[k][:, width:]
                            outs[q + d - 2][j] = parts[k][:, first:width]

        sent = kernel_call(
            pick,
            ints,
            held,
            [jax.ShapeDtypeStruct((seqs, rank, first + cols), BF16)] * (q - 1)
            + [jax.ShapeDtypeStruct((seqs, rank, rest), BF16)] * (q - 1),
        )
        got = [[], []]
        for p in range(2):
            for d in range(1, q):
                got[p].append(send_inner(sent[p * (q - 1) + d - 1], d))

        def chosen(refs, from_peer, from_held):
            ins, parts, gots = refs[: 2 + q], refs[2 + q : 2 + q + r], refs[2 + q + r : 1 + 2 * q + r]
            inner, outer = ins[0][0] % q, ins[0][0] // q
            for j in range(seqs):
                wanted = slot(ins, 0, j)
                way = offset(inner, wanted % q, q)
                have = offset(outer, wanted // q, r)
                for d in range(1, q):

                    @pl.when(way == d)
                    def _(d=d, j=j):
                        from_peer(j, gots[d - 1].at[j])

                for k in range(r):

                    @pl.when((way == 0) & (have == k))
                    def _(j=j, k=k):
                        from_held(j, parts[k])

        def choose0(*refs):
            down_out, up_out = refs[-2:]

            def from_peer(j, ref):
                down_out[j] = ref[:, :first]
                up_out[j] = ref[:, first:]

            def from_held(j, ref):
                down_out[j] = ref[:, :first]
                up_out[j] = ref[:, width:]

            chosen(refs, from_peer, from_held)

        def choose1(*refs):
            down_in, down_out = refs[-2:]
            down_out[:, :, :first] = down_in[...]

            def from_peer(j, ref):
                down_out[j, :, first:] = ref[...]

            def from_held(j, ref):
                down_out[j, :, first:] = ref[:, first:width]

            chosen(refs, from_peer, from_held)

        down_first, up_s = kernel_call(
            choose0,
            ints,
            held + got[0],
            [jax.ShapeDtypeStruct((seqs, rank, first), BF16), jax.ShapeDtypeStruct((seqs, rank, cols), BF16)],
        )
        (down_s,) = kernel_call(
            choose1, ints, held + got[1] + [down_first], [jax.ShapeDtypeStruct((seqs, rank, width), BF16)]
        )

        h3 = hidden.reshape(seqs, length, width)
        g3 = grad_in.reshape(seqs, length, cols)
        if m == 2:
            other = swap(grad_in)
        else:
            grad_full = lax.all_gather(grad, "mp", axis=1, tiled=True)
        if m == 2:
            both = jnp.where(
                low_core, jnp.concatenate([grad_in, other], axis=1), jnp.concatenate([other, grad_in], axis=1)
            )
            pre = lax.dot_general(both, weight, (((1,), (1,)), ((), ())), preferred_element_type=F32)
            pre = pltpu.with_memory_space_constraint(pre, pltpu.VMEM)
        base = []
        for j in range(seqs):
            base.append(jnp.dot(h3[j], weight, preferred_element_type=F32))
        if m == 2:
            theirs = jnp.concatenate([jnp.where(low_core, x[:, cols:], x[:, :cols]) for x in base])
            base_got = swap(theirs)
        else:
            base_own = lax.psum_scatter(jnp.concatenate(base), "mp", scatter_dimension=1, tiled=True)

        back_low = mp_sum(jnp.einsum("slk,srk->srl", g3, up_s, preferred_element_type=F32)).astype(BF16)
        low = mp_sum(jnp.einsum("slw,srw->srl", h3, down_s, preferred_element_type=F32))
        up_seq = jnp.einsum("srl,slk->srk", low, g3.astype(F32), precision=HIGH)
        down_seq = jnp.einsum("srl,slw->srw", back_low, h3, preferred_element_type=F32)
        if m == 2:
            per = length // block

            def outputs(core_ref, pre_ref, coeff, factor, low_ref, up_ref, got_ref, *rest_refs):
                bases, (out, values_out) = rest_refs[:seqs], rest_refs[seqs:]
                step = pl.program_id(0)
                here = pl.multiple_of(core_ref[0] * cols, math.gcd(cols, 128))
                out[...] = (
                    pre_ref[pl.ds(pl.multiple_of(step * block, block), block), :]
                    + lax.dot_general(
                        coeff[0], factor[0], (((0,), (0,)), ((), ())), preferred_element_type=F32
                    )
                ).astype(BF16)
                term = got_ref[...] + lax.dot_general(
                    low_ref[0],
                    up_ref[0].astype(F32),
                    (((0,), (0,)), ((), ())),
                    precision=HIGH,
                    preferred_element_type=F32,
                )
                for j in range(seqs):

                    @pl.when(step // per == j)
                    def _(j=j):
                        at = pl.multiple_of(step % per * block, block)
                        values_out[...] = (term + bases[j][pl.ds(at, block), pl.ds(here, cols)]).astype(BF16)

            rows_of = pl.BlockSpec((block, cols), lambda i: (i, 0))
            coeff_of = pl.BlockSpec((1, rank, block), lambda i: (i // per, 0, i % per))
            values, hidden_grad = pl.pallas_call(
                outputs,
                grid=(rows // block,),
                out_shape=[
                    jax.ShapeDtypeStruct((rows, width), BF16),
                    jax.ShapeDtypeStruct((rows, cols), BF16),
                ],
                in_specs=[
                    SMEM,
                    VMEM,
                    coeff_of,
                    pl.BlockSpec((1, rank, width), lambda i: (i // per, 0, 0)),
                    coeff_of,
                    pl.BlockSpec((1, rank, cols), lambda i: (i // per, 0, 0)),
                    rows_of,
                ]
                + [VMEM] * seqs,
                out_specs=[pl.BlockSpec((block, width), lambda i: (i, 0)), rows_of],
                compiler_params=pltpu.CompilerParams(vmem_limit_bytes=32 << 20),
                name="outputs",
            )(core, pre, back_low, down_s, low, up_s, base_got, *base)[::-1]
        else:
            values = (
                base_own.reshape(seqs, length, cols)
                + jnp.einsum("srl,srk->slk", low, up_s.astype(F32), precision=HIGH)
            ).astype(BF16)
            hidden_grad = (
                lax.dot_general(grad_full, weight, (((1,), (1,)), ((), ())), preferred_element_type=F32)
                + jnp.einsum("srl,srw->slw", back_low, down_s, preferred_element_type=F32).reshape(rows, width)
            ).astype(BF16)

        early = (width + cols) * 5 // 1024 * 128
        items = [down_seq[:, :, :early], jnp.concatenate([down_seq[:, :, early:], up_seq], axis=2)]
        near = [[], []]
        for p in range(2):
            small = items[p].astype(BF16)
            for d in range(1, q):
                near[p].append(send_inner(small, d))

        def gather_items(*refs):
            ins, own, others = refs[: 2 + q], refs[2 + q], refs[3 + q : 2 + 2 * q]
            outs, acc = refs[2 + 2 * q : -1], refs[-1]
            inner, outer = ins[0][0] % q, ins[0][0] // q
            acc[...] = jnp.zeros_like(acc)
            for d in range(q):
                for j in range(seqs):
                    holder = slot(ins, d, j)

                    @pl.when(holder % q == inner)
                    def _(d=d, j=j, holder=holder):
                        k = offset(outer, holder // q, r)
                        item = own[j] if d == 0 else others[d - 1][j].astype(F32)
                        acc[k] += item

            outs[0][...] = acc[0]
            for k in range(1, r):
                outs[k][...] = acc[k].astype(BF16)

        totals, arrived = [], []
        for p in range(2):
            shape = items[p].shape[1:]
            parts = kernel_call(
                gather_items,
                ints,
                [items[p]] + near[p],
                [jax.ShapeDtypeStruct(shape, F32)] + [jax.ShapeDtypeStruct(shape, BF16)] * (r - 1),
                [pltpu.VMEM((r,) + shape, F32)],
            )
            totals.append(parts[0])
            for k in range(1, r):
                arrived.append(send_outer(parts[k], opposite(k, r)))
        values, hidden_grad, arrived = lax.optimization_barrier((values, hidden_grad, arrived))

        def finish(*refs):
            own, others, down_out, up_out = refs[:2], refs[2 : 2 * r], refs[2 * r], refs[2 * r + 1]
            total = [own[0][...], own[1][...]]
            for p in range(2):
                for other in others[p * (r - 1) : (p + 1) * (r - 1)]:
                    total[p] = total[p] + other[...].astype(F32)
            down_out[:, :early] = total[0]
            down_out[:, early:] = total[1][:, : width - early]
            up_out[...] = total[1][:, width - early :]

        down_grad, up_grad = kernel_call(
            finish,
            [],
            totals + arrived,
            [jax.ShapeDtypeStruct((rank, width), F32), jax.ShapeDtypeStruct((rank, cols), F32)],
            inside=False,
        )
        down_grad = jnp.swapaxes(down_grad, 0, 1)[None]
        return values.reshape(rows, cols), hidden_grad, down_grad, up_grad[None]

    return local


def solution(mesh):
    n, m = mesh.shape["dp"], mesh.shape["mp"]
    return jax.shard_map(
        program(n, m),
        mesh=mesh,
        in_specs=(
            P("dp", "mp"),
            P("mp", None),
            P("dp", "mp", None),
            P("dp", None, "mp"),
            P("dp", "mp"),
            P("dp"),
            P(),
        ),
        out_specs=(P("dp", "mp"), P("dp", "mp"), P("dp", "mp", None), P("dp", None, "mp")),
        check_vma=False,
    )
```

```python
import math

import jax
import jax.numpy as jnp
from jax import lax
from jax.experimental import pallas as pl
from jax.experimental.pallas import tpu as pltpu
from jax.sharding import PartitionSpec as P


HIGH = lax.Precision.HIGHEST
F32 = jnp.float32
BF16 = jnp.bfloat16


def inner_size(n):
    return max(q for q in range(1, n + 1) if n % q == 0 and q * q <= n)


def peer(i, d, n):
    return i ^ d if n & (n - 1) == 0 else (i + d) % n


def offset(dst, src, n):
    return dst ^ src if n & (n - 1) == 0 else (dst - src) % n


SMEM = pl.BlockSpec(memory_space=pltpu.SMEM)
VMEM = pl.BlockSpec(memory_space=pltpu.VMEM)
SMALL = pltpu.CompilerParams(vmem_limit_bytes=8 << 20)


def fixed(x):
    return pltpu.with_memory_space_constraint(x, pltpu.HBM)


def kernel_call(body, ints, arrays, outs, scratch=(), inside=True):
    arrays = [pltpu.with_memory_space_constraint(a, pltpu.VMEM) for a in arrays]
    return pl.pallas_call(
        body,
        out_shape=[pltpu.VMEM(o.shape, o.dtype) if inside else o for o in outs],
        in_specs=[SMEM] * len(ints) + [VMEM] * len(arrays),
        out_specs=[VMEM] * len(outs),
        scratch_shapes=list(scratch),
        compiler_params=SMALL,
    )(*ints, *arrays)


def program(n, m):
    q = inner_size(n)
    r = n // q

    def send_inner(x, d):
        return lax.ppermute(x, "dp", [(i, i // q * q + peer(i % q, d, q)) for i in range(n)])

    def send_outer(x, d):
        return lax.ppermute(x, "dp", [(i, peer(i // q, d, r) * q + i % q) for i in range(n)])

    def swap(x):
        return lax.ppermute(x, "mp", [(0, 1), (1, 0)])

    def mp_sum(x):
        return x + swap(x) if m == 2 else lax.psum(x, "mp")

    def opposite(d, size):
        return d if size & (size - 1) == 0 else (size - d) % size

    def local(hidden, weight, down, up, grad, tenant, table):
        seqs = tenant.shape[0]
        rows, width = hidden.shape
        rank = down.shape[2]
        cols = grad.shape[1]
        length = rows // seqs
        block = math.gcd(length, 768)
        me = lax.axis_index("dp").astype(jnp.int32)[None]
        core = lax.axis_index("mp").astype(jnp.int32)[None]
        low_core = lax.axis_index("mp") == 0
        me, core, low_core, down, up, tenant = lax.optimization_barrier((me, core, low_core, down, up, tenant))

        first = max(width * 512 // 1792 // 128 * 128, 128)
        rest = width - first

        def join(down_ref, up_ref, out):
            out[:, :width] = down_ref[...]
            out[:, width:] = up_ref[...]

        mine = pl.pallas_call(
            join,
            out_shape=pltpu.VMEM((rank, width + cols), BF16),
            compiler_params=SMALL,
            name="join",
        )(fixed(jnp.swapaxes(down[0], 0, 1)), fixed(up[0]))
        held, tenants = [mine], [tenant]
        for d in range(1, r):
            held.append(send_outer(mine, d))
        for d in range(1, q):
            tenants.append(send_inner(tenant, d))
        ints = [me, table, tenant] + tenants[1:]

        def load(x_ref, g_ref, x_out, g_out, sems):
            copies = [
                pltpu.make_async_copy(x_ref, x_out, sems.at[0]),
                pltpu.make_async_copy(g_ref, g_out, sems.at[1]),
            ]
            for c in copies:
                c.start()
            for c in copies:
                c.wait()

        hidden, grad_in = pl.pallas_call(
            load,
            out_shape=[pltpu.VMEM(hidden.shape, BF16), pltpu.VMEM(grad.shape, BF16)],
            in_specs=[pl.BlockSpec(memory_space=pl.ANY)] * 2,
            out_specs=[VMEM] * 2,
            scratch_shapes=[pltpu.SemaphoreType.DMA((2,))],
            compiler_params=SMALL,
            name="load",
        )(fixed(hidden), fixed(grad))

        def slot(refs, d, j):
            return refs[1][refs[2 + d][j]]

        def pick(*refs):
            ins, parts, outs = refs[: 2 + q], refs[2 + q : 2 + q + r], refs[2 + q + r :]
            outer = ins[0][0] // q
            for d in range(1, q):
                for j in range(seqs):
                    have = offset(outer, slot(ins, opposite(d, q), j) // q, r)
                    for k in range(r):

                        @pl.when(have == k)
                        def _(d=d, j=j, k=k):
                            outs[d - 1][j, :, :first] = parts[k][:, :first]
                            outs[d - 1][j, :, first:] = parts[k][:, width:]
                            outs[q + d - 2][j] = parts[k][:, first:width]

        sent = kernel_call(
            pick,
            ints,
            held,
            [jax.ShapeDtypeStruct((seqs, rank, first + cols), BF16)] * (q - 1)
            + [jax.ShapeDtypeStruct((seqs, rank, rest), BF16)] * (q - 1),
        )
        got = [[], []]
        for p in range(2):
            for d in range(1, q):
                got[p].append(send_inner(sent[p * (q - 1) + d - 1], d))

        def chosen(refs, from_peer, from_held):
            ins, parts, gots = refs[: 2 + q], refs[2 + q : 2 + q + r], refs[2 + q + r : 1 + 2 * q + r]
            inner, outer = ins[0][0] % q, ins[0][0] // q
            for j in range(seqs):
                wanted = slot(ins, 0, j)
                way = offset(inner, wanted % q, q)
                have = offset(outer, wanted // q, r)
                for d in range(1, q):

                    @pl.when(way == d)
                    def _(d=d, j=j):
                        from_peer(j, gots[d - 1].at[j])

                for k in range(r):

                    @pl.when((way == 0) & (have == k))
                    def _(j=j, k=k):
                        from_held(j, parts[k])

        def choose0(*refs):
            down_out, up_out = refs[-2:]

            def from_peer(j, ref):
                down_out[j] = ref[:, :first]
                up_out[j] = ref[:, first:]

            def from_held(j, ref):
                down_out[j] = ref[:, :first]
                up_out[j] = ref[:, width:]

            chosen(refs, from_peer, from_held)

        def choose1(*refs):
            down_in, down_out = refs[-2:]
            down_out[:, :, :first] = down_in[...]

            def from_peer(j, ref):
                down_out[j, :, first:] = ref[...]

            def from_held(j, ref):
                down_out[j, :, first:] = ref[:, first:width]

            chosen(refs, from_peer, from_held)

        down_first, up_s = kernel_call(
            choose0,
            ints,
            held + got[0],
            [jax.ShapeDtypeStruct((seqs, rank, first), BF16), jax.ShapeDtypeStruct((seqs, rank, cols), BF16)],
        )
        (down_s,) = kernel_call(
            choose1, ints, held + got[1] + [down_first], [jax.ShapeDtypeStruct((seqs, rank, width), BF16)]
        )

        h3 = hidden.reshape(seqs, length, width)
        g3 = grad_in.reshape(seqs, length, cols)
        if m == 2:
            other = swap(grad_in)
        else:
            grad_full = lax.all_gather(grad, "mp", axis=1, tiled=True)
        if m == 2:
            both = jnp.where(
                low_core, jnp.concatenate([grad_in, other], axis=1), jnp.concatenate([other, grad_in], axis=1)
            )
            both = both.reshape(seqs, length, m * cols)
            pre = []
            for j in range(seqs):
                pre.append(lax.dot_general(both[j], weight, (((1,), (1,)), ((), ())), preferred_element_type=F32))
            pre = [pltpu.with_memory_space_constraint(x, pltpu.VMEM) for x in pre]
        base = []
        for j in range(seqs):
            base.append(jnp.dot(h3[j], weight, preferred_element_type=F32))
        if m == 2:
            theirs = jnp.concatenate([jnp.where(low_core, x[:, cols:], x[:, :cols]) for x in base])
            base_got = swap(theirs)
        else:
            base_own = lax.psum_scatter(jnp.concatenate(base), "mp", scatter_dimension=1, tiled=True)

        back_low = mp_sum(jnp.einsum("slk,srk->srl", g3, up_s, preferred_element_type=F32)).astype(BF16)
        low = mp_sum(jnp.einsum("slw,srw->srl", h3, down_s, preferred_element_type=F32))
        up_seq = jnp.einsum("srl,slk->srk", low, g3.astype(F32), precision=HIGH)
        down_seq = jnp.einsum("srl,slw->srw", back_low, h3, preferred_element_type=F32)
        if m == 2:
            per = length // block

            def outputs(core_ref, coeff, factor, low_ref, up_ref, got_ref, *rest_refs):
                pres, bases, (out, values_out) = rest_refs[:seqs], rest_refs[seqs : 2 * seqs], rest_refs[2 * seqs :]
                step = pl.program_id(0)
                at = pl.multiple_of(step % per * block, block)
                here = pl.multiple_of(core_ref[0] * cols, math.gcd(cols, 128))
                piece, parts = low_ref[0], []
                for _ in range(3):
                    parts.append(piece.astype(BF16))
                    piece = piece - parts[-1].astype(F32)
                term = got_ref[...] + lax.dot_general(
                    jnp.concatenate(parts, axis=0),
                    jnp.concatenate([up_ref[0]] * 3, axis=0),
                    (((0,), (0,)), ((), ())),
                    preferred_element_type=F32,
                )
                for j in range(seqs):

                    @pl.when(step // per == j)
                    def _(j=j):
                        adapter = lax.dot_general(
                            coeff[0], factor[0], (((0,), (0,)), ((), ())), preferred_element_type=F32
                        )
                        out[...] = (adapter + pres[j][pl.ds(at, block), :]).astype(BF16)
                        values_out[...] = (term + bases[j][pl.ds(at, block), pl.ds(here, cols)]).astype(BF16)

            rows_of = pl.BlockSpec((block, cols), lambda i: (i, 0))
            coeff_of = pl.BlockSpec((1, rank, block), lambda i: (i // per, 0, i % per))
            values, hidden_grad = pl.pallas_call(
                outputs,
                grid=(rows // block,),
                out_shape=[
                    jax.ShapeDtypeStruct((rows, width), BF16),
                    jax.ShapeDtypeStruct((rows, cols), BF16),
                ],
                in_specs=[
                    SMEM,
                    coeff_of,
                    pl.BlockSpec((1, rank, width), lambda i: (i // per, 0, 0)),
                    coeff_of,
                    pl.BlockSpec((1, rank, cols), lambda i: (i // per, 0, 0)),
                    rows_of,
                ]
                + [VMEM] * (2 * seqs),
                out_specs=[pl.BlockSpec((block, width), lambda i: (i, 0)), rows_of],
                compiler_params=pltpu.CompilerParams(vmem_limit_bytes=32 << 20),
                name="outputs",
            )(core, back_low, down_s, low, up_s, base_got, *pre, *base)[::-1]
        else:
            values = (
                base_own.reshape(seqs, length, cols)
                + jnp.einsum("srl,srk->slk", low, up_s.astype(F32), precision=HIGH)
            ).astype(BF16)
            hidden_grad = (
                lax.dot_general(grad_full, weight, (((1,), (1,)), ((), ())), preferred_element_type=F32)
                + jnp.einsum("srl,srw->slw", back_low, down_s, preferred_element_type=F32).reshape(rows, width)
            ).astype(BF16)

        early = (width + cols) * 9 // 2048 * 128
        items = [down_seq[:, :, :early], jnp.concatenate([down_seq[:, :, early:], up_seq], axis=2)]
        near = [[], []]
        for p in range(2):
            small = items[p].astype(BF16)
            for d in range(1, q):
                near[p].append(send_inner(small, d))

        def gather_items(*refs):
            ins, own, others = refs[: 2 + q], refs[2 + q], refs[3 + q : 2 + 2 * q]
            outs, acc = refs[2 + 2 * q : -1], refs[-1]
            inner, outer = ins[0][0] % q, ins[0][0] // q
            acc[...] = jnp.zeros_like(acc)
            for d in range(q):
                for j in range(seqs):
                    holder = slot(ins, d, j)

                    @pl.when(holder % q == inner)
                    def _(d=d, j=j, holder=holder):
                        k = offset(outer, holder // q, r)
                        item = own[j] if d == 0 else others[d - 1][j].astype(F32)
                        acc[k] += item

            outs[0][...] = acc[0]
            for k in range(1, r):
                outs[k][...] = acc[k].astype(BF16)

        totals, arrived = [], []
        for p in range(2):
            shape = items[p].shape[1:]
            parts = kernel_call(
                gather_items,
                ints,
                [items[p]] + near[p],
                [jax.ShapeDtypeStruct(shape, F32)] + [jax.ShapeDtypeStruct(shape, BF16)] * (r - 1),
                [pltpu.VMEM((r,) + shape, F32)],
            )
            totals.append(parts[0])
            for k in range(1, r):
                arrived.append(send_outer(parts[k], opposite(k, r)))
        values, hidden_grad, arrived = lax.optimization_barrier((values, hidden_grad, arrived))

        def finish(*refs):
            own, others, down_out, up_out = refs[:2], refs[2 : 2 * r], refs[2 * r], refs[2 * r + 1]
            total = [own[0][...], own[1][...]]
            for p in range(2):
                for other in others[p * (r - 1) : (p + 1) * (r - 1)]:
                    total[p] = total[p] + other[...].astype(F32)
            down_out[:, :early] = total[0]
            down_out[:, early:] = total[1][:, : width - early]
            up_out[...] = total[1][:, width - early :]

        down_grad, up_grad = kernel_call(
            finish,
            [],
            totals + arrived,
            [jax.ShapeDtypeStruct((rank, width), F32), jax.ShapeDtypeStruct((rank, cols), F32)],
            inside=False,
        )
        down_grad = jnp.swapaxes(down_grad, 0, 1)[None]
        return values.reshape(rows, cols), hidden_grad, down_grad, up_grad[None]

    return local


def solution(mesh):
    n, m = mesh.shape["dp"], mesh.shape["mp"]
    return jax.shard_map(
        program(n, m),
        mesh=mesh,
        in_specs=(
            P("dp", "mp"),
            P("mp", None),
            P("dp", "mp", None),
            P("dp", None, "mp"),
            P("dp", "mp"),
            P("dp"),
            P(),
        ),
        out_specs=(P("dp", "mp"), P("dp", "mp"), P("dp", "mp", None), P("dp", None, "mp")),
        check_vma=False,
    )
```
